32 devices in a mesh: unit: 4 (over y, core), zero: 4 (over z), cols: 2 (over x).
Axes of the slice: x: 2, y: 2, z: 4, core: 2. Of those that a mesh axis runs over, the one named last changes fastest.
Arguments:
- weight_gate: bfloat16 [20480, 13824], P(('unit', 'zero'), 'cols'), parts along dimension 0, may hold values from -0.125 to 0.125
- low_gate: bfloat16 [20480, 32], P(('unit', 'zero')), parts along dimension 0, may hold values from -0.078125 to 0.078125
- high_gate: bfloat16 [128, 13824], P('unit', 'cols'), parts along dimension 0, may hold values from -1 to 1
- weight_up: bfloat16 [20480, 13824], P(('unit', 'zero'), 'cols'), parts along dimension 0, may hold values from -0.125 to 0.125
- low_up: bfloat16 [20480, 32], P(('unit', 'zero')), parts along dimension 0, may hold values from -0.078125 to 0.078125
- high_up: bfloat16 [128, 13824], P('unit', 'cols'), parts along dimension 0, may hold values from -1 to 1
- norm_train: float32 [20480], P(('unit', 'zero', 'cols')), parts along dimension 0, may hold values from 0.25 to 1.75
- norm_step: float32 [20480], P(('unit', 'zero', 'cols')), parts along dimension 0, may hold values from -0.3 to 0.3
Outputs:
- final_gate: bfloat16 [20480, 13824], P('unit', ('cols', 'zero')), parts along dimension 0
- final_up: bfloat16 [20480, 13824], P('unit', ('cols', 'zero')), parts along dimension 0
- scale_gate: float32 [55296], P(('unit', 'cols', 'zero')), parts along dimension 0
- scale_up: float32 [55296], P(('unit', 'cols', 'zero')), parts along dimension 0
- serve_norm: bfloat16 [20480], P('unit'), parts along dimension 0
The draws below stay inside these ranges and needn't reach their ends.
There are 4 independent parts, one for each index of `unit`. The reference program is written for one: setup_inputs(seed, part) draws one part's arguments, and reference() takes and returns one part's arrays. A program takes and returns all parts, laid end to end along the dimension named above; each array names one. Nothing has to cross between parts.
All inputs are finite; a program needn't handle non-finite values. Where the reference program divides by a largest or mean magnitude, that divisor is 1e-20 or more.
Results may differ from the reference program's by a relative error of at most 0.001.
Values may be sent and summed in bfloat16 or wider, within the bound.
A program may use at most 192 MiB of HBM per device.

```python
import jax
import jax.numpy as jnp

D_MODEL = 5120
D_INNER = 13824
RANK = 32


def strengthened(entries, own_key, source, target, parts, factor):
    def block_of(position):
        return (jnp.arange(entries.shape[position]) // (entries.shape[position] // parts)).reshape((-1,) + (1,) * (entries.ndim - 1 - position))

    one_side = jax.random.permutation(own_key, parts)[block_of(target)]
    other_side = (block_of(target) + parts // 2) % parts
    return jnp.where((block_of(source) == one_side) | (block_of(source) == other_side), factor * entries, entries)


def levels(own_key, extent, split, least, top_value):
    level, own = 1.0, jax.random.fold_in(own_key, 6)
    for dim, blocks in split:
        draws = jnp.exp(jax.random.uniform(jax.random.fold_in(own, dim), (blocks,), jnp.float32, least / len(split), top_value / len(split)))
        level = level * jnp.repeat(draws, extent[dim] // blocks).reshape([-1 if axis == dim else 1 for axis in range(len(extent))])
    return level


def normal_values(rng, extent, deviation, most, cuts=(), kind=jnp.bfloat16):
    level = levels(rng, extent, cuts, -0.22, 0.18) if cuts else 1.0
    entries = jax.random.normal(rng, extent, jnp.float32) * deviation * level
    return jnp.minimum(jnp.maximum(entries, -most), most).astype(kind)


def gaussian_with(stream_key, extent, width, bound, shards, heavy, held_as=jnp.bfloat16):
    values = width * jax.random.normal(stream_key, extent, jnp.float32)
    if shards:
        values = values * levels(stream_key, extent, shards, -0.22, 0.18)
    return jnp.clip(strengthened(values, jax.random.fold_in(stream_key, 3), *heavy), -bound, bound).astype(held_as)


def setup_inputs(seed: int = 0, part: int = 0) -> dict:
    keys = jax.random.split(jax.random.key(seed), 9)
    part_splits = jax.random.split(jax.random.fold_in(keys[8], part), 9)
    return {
        "weight_gate": gaussian_with(part_splits[0], (D_MODEL, D_INNER), D_MODEL ** -0.5, 0.125, ((0, 4), (1, 2)), (0, 1, 4, 2.0)),
        "low_gate": normal_values(part_splits[1], (D_MODEL, RANK), D_MODEL ** -0.5, 0.078125, ((0, 4),)),
        "high_gate": normal_values(part_splits[2], (RANK, D_INNER), RANK ** -0.5, 1.0, ((1, 2),)),
        "weight_up": gaussian_with(part_splits[3], (D_MODEL, D_INNER), D_MODEL ** -0.5, 0.125, ((0, 4), (1, 2)), (0, 1, 4, 2.0)),
        "low_up": normal_values(part_splits[4], (D_MODEL, RANK), D_MODEL ** -0.5, 0.078125, ((0, 4),)),
        "high_up": normal_values(part_splits[5], (RANK, D_INNER), RANK ** -0.5, 1.0, ((1, 2),)),
        "norm_train": jnp.clip(1.0 + 0.15 * jax.random.normal(part_splits[6], (D_MODEL,), jnp.float32), 0.25, 1.75),
        "norm_step": jnp.clip(jax.random.uniform(part_splits[7], (D_MODEL,), jnp.float32, -0.3, 0.3) * levels(part_splits[7], (D_MODEL,), ((0, 8),), -0.4, 0.0), -0.3, 0.3),
    }


mix_rate = 0.5


def reference(weight_gate, low_gate, high_gate, weight_up, low_up, high_up, norm_train, norm_step):
    result_gate = weight_gate.astype(jnp.float32) + mix_rate * jnp.dot(low_gate, high_gate, preferred_element_type=jnp.float32)
    result_up = weight_up.astype(jnp.float32) + mix_rate * jnp.dot(low_up, high_up, preferred_element_type=jnp.float32)
    scale_gate = jnp.sum(jnp.abs(result_gate), axis=0) / D_MODEL
    final_gate = (result_gate / scale_gate).astype(jnp.bfloat16)
    scale_up = jnp.sum(jnp.abs(result_up), axis=0) / D_MODEL
    final_up = (result_up / scale_up).astype(jnp.bfloat16)
    serve_norm = (norm_train + norm_step).astype(jnp.bfloat16)
    return final_gate, final_up, scale_gate, scale_up, serve_norm
```

```python
import functools

import jax
import jax.numpy as jnp
from jax import lax
from jax.experimental import pallas as pl
from jax.experimental.pallas import tpu as pltpu
from jax.sharding import PartitionSpec as P

mix_rate = 0.5


def cuts(units, shares):
    total, marks, seen = sum(shares), [0], 0
    for share in shares:
        seen += share
        marks.append(units * seen // total)
    return [(a, b) for a, b in zip(marks[:-1], marks[1:]) if b > a]


def merge_kernel(block_ref, low_ref, high_ref, *refs):
    final_ref, scale_ref, result_ref = refs[-3:]
    n, _, rows = block_ref.shape
    change = mix_rate * jnp.dot(high_ref[...], low_ref[...], preferred_element_type=jnp.float32)
    total = None
    for s in range(n):
        part = block_ref[s].astype(jnp.float32) + change[:, s * rows : (s + 1) * rows]
        result_ref[:, s * rows : (s + 1) * rows] = part
        size = jnp.sum(jnp.abs(part), axis=1, keepdims=True)
        total = size if total is None else total + size
    scale = total / (n * rows)
    scale_ref[...] = scale
    final_ref[...] = (result_ref[...] / scale).astype(final_ref.dtype)


def merge(block, low, high, final, first, step, width):
    n, part, rows = block.shape
    rank = low.shape[0]
    offset = first // step
    operands = [block, low, high]
    in_specs = [
        pl.BlockSpec((n, step, rows), lambda i: (0, i, 0)),
        pl.BlockSpec((rank, n * rows), lambda i: (0, 0)),
        pl.BlockSpec((step, rank), lambda i: (i + offset, 0)),
    ]
    aliases = {}
    if final is not None:
        operands.append(final)
        in_specs.append(pl.BlockSpec(memory_space=pl.ANY))
        aliases = {3: 0}
    return pl.pallas_call(
        merge_kernel,
        grid=(part // step,),
        in_specs=in_specs,
        out_specs=[
            pl.BlockSpec((step, n * rows), lambda i: (i + offset, 0)),
            pl.BlockSpec((step, 1), lambda i: (i, 0)),
        ],
        out_shape=[
            jax.ShapeDtypeStruct((width, n * rows), jnp.bfloat16),
            jax.ShapeDtypeStruct((part, 1), jnp.float32),
        ],
        scratch_shapes=[pltpu.VMEM((step, n * rows), jnp.float32)],
        input_output_aliases=aliases,
        cost_estimate=pl.CostEstimate(
            flops=2 * part * n * rows * rank,
            bytes_accessed=4 * part * n * rows,
            transcendentals=0,
        ),
        compiler_params=pltpu.CompilerParams(vmem_limit_bytes=24 << 20),
    )(*operands)


def general(weight_gate, low_gate, high_gate, weight_up, low_up, high_up, norm_train, norm_step):
    n = lax.axis_size("zero")
    rows, width = weight_gate.shape[0], weight_gate.shape[1] // n
    rank = low_gate.shape[1]
    place = lax.axis_index("zero")
    step = next(s for s in (48, 24, 16, 8, width) if width % s == 0)

    lows = lax.all_gather(
        jnp.concatenate([low_gate.T, low_up.T], axis=0), "zero", axis=1, tiled=True
    )
    serve_norm = lax.all_gather(
        (norm_train + norm_step).astype(jnp.bfloat16), ("zero", "cols"), axis=0, tiled=True
    )
    lows, serve_norm, weight_gate, weight_up = lax.optimization_barrier(
        (lows, serve_norm, weight_gate, weight_up)
    )
    low = {"gate": lows[:rank], "up": lows[rank:]}
    high = {
        "gate": lax.dynamic_slice_in_dim(high_gate, place * width, width, axis=1).T,
        "up": lax.dynamic_slice_in_dim(high_up, place * width, width, axis=1).T,
    }
    turned = {
        "gate": weight_gate.T.reshape(n, width, rows),
        "up": weight_up.T.reshape(n, width, rows),
    }

    shares = {"gate": (1, 3), "up": (7, 2)}
    jobs = [
        (name, a * step, b * step)
        for name in ("gate", "up")
        for a, b in cuts(width // step, shares[name])
    ]
    finals = {"gate": None, "up": None}
    scales = {"gate": [], "up": []}
    block = None
    arrived = []
    for name, a, b in jobs:
        sent = turned[name][:, a:b]
        if block is not None:
            sent, block = lax.optimization_barrier((sent, block))
            arrived.append(block)
        block = lax.all_to_all(sent, "zero", split_axis=0, concat_axis=0, tiled=True)
    arrived.append(block)
    for (name, a, b), block in zip(jobs, arrived):
        finals[name], scale = merge(block, low[name], high[name], finals[name], a, step, width)
        scales[name].append(scale[:, 0])
    return (
        finals["gate"].T,
        finals["up"].T,
        jnp.concatenate(scales["gate"]),
        jnp.concatenate(scales["up"]),
        serve_norm,
    )


MESH = pl.DeviceIdType.MESH
LANES, HALF, AHEAD = 128, 64, 4
SLOTS = AHEAD + 2


def exchange_kernel(
    n, groups,
    weight_gate, weight_up, low_gate, low_up, high_gate, high_up, norm_train, norm_step,
    final, scales, norms,
    raw, raw_pair, sent, sent_pair, lows, highs, turned, result, train, step, sums,
    raw_sem, pair_sem, low_sem, high_sem, norm_sem,
    send_sem, recv_sem, pair_send, pair_recv, low_send, low_recv, swap_sem, norm_send, norm_recv,
):
    rows, total = weight_gate.shape
    width = total // n
    rank = low_gate.shape[0]
    mains = width // LANES
    steps = 2 * mains
    weights, own_lows, own_highs = (weight_gate, weight_up), (low_gate, low_up), (high_gate, high_up)
    z, x = lax.axis_index("zero"), lax.axis_index("cols")
    odd = lax.rem(z, 2)
    here = z * groups + x
    lanes = pl.ds(pl.multiple_of(z * rows, LANES), rows)

    def peer(shift):
        return lax.rem(z + shift, n)

    def first_row(d):
        return HALF * lax.rem(d, 2)

    def pair_row(d):
        return (width - HALF) * (1 - lax.rem(d, 2))

    def load(a, s, slot, j):
        d = peer(j)
        tile = (d // 2) * (2 * width // LANES) + lax.rem(d, 2) * (mains + 1) + s
        start = pl.multiple_of(tile * LANES, LANES)
        return pltpu.make_async_copy(
            weights[a].at[:, pl.ds(start, LANES)], raw.at[slot, j], raw_sem.at[slot, j]
        )

    def start_loads(t):
        for a in range(2):
            def go(a=a):
                for j in range(n):
                    load(a, t - a * mains, lax.rem(t, 2), j).start()
            if isinstance(t, int):
                if t // mains == a:
                    go()
            else:
                pl.when(t // mains == a)(go)

    def load_pair(a, q):
        tile = q * (2 * width // LANES) + mains
        return pltpu.make_async_copy(
            weights[a].at[:, pl.ds(tile * LANES, LANES)], raw_pair.at[a, q], pair_sem.at[a, q]
        )

    def own_low(a):
        return pltpu.make_async_copy(own_lows[a], lows.at[a, z], low_sem)

    def own_high(a):
        start = pl.multiple_of(z * width - HALF * odd, LANES)
        return pltpu.make_async_copy(
            own_highs[a].at[:, pl.ds(start, width + HALF)], highs.at[a], high_sem.at[a]
        )

    def bulk(t, j):
        d = peer(j)
        a = t // mains
        row = pl.multiple_of(first_row(d) + LANES * (t - a * mains), HALF)
        slot = lax.rem(t, SLOTS)
        return pltpu.make_async_remote_copy(
            src_ref=sent.at[slot, j - 1],
            dst_ref=final.at[a, pl.ds(row, LANES), lanes],
            send_sem=send_sem.at[slot, j - 1],
            recv_sem=recv_sem.at[t, j - 1],
            device_id={"zero": d},
            device_id_type=MESH,
        )

    def pair(a, j):
        d = peer(j)
        return pltpu.make_async_remote_copy(
            src_ref=sent_pair.at[a, d // 2, pl.ds(pl.multiple_of(first_row(d), HALF), HALF)],
            dst_ref=final.at[a, pl.ds(pl.multiple_of(pair_row(d), HALF), HALF), lanes],
            send_sem=pair_send.at[a, j - 1],
            recv_sem=pair_recv.at[a, j - 1],
            device_id={"zero": d},
            device_id_type=MESH,
        )

    def low_copy(block, d, index):
        return pltpu.make_async_remote_copy(
            src_ref=lows.at[x, block],
            dst_ref=lows.at[x, block],
            send_sem=low_send.at[index],
            recv_sem=low_recv.at[block],
            device_id={"zero": d},
            device_id_type=MESH,
        )

    def low_swap():
        return pltpu.make_async_remote_copy(
            src_ref=lows.at[x],
            dst_ref=lows.at[x],
            send_sem=swap_sem.at[0],
            recv_sem=swap_sem.at[1],
            device_id={"cols": 1 - x},
            device_id_type=MESH,
        )

    def norm_copy(i):
        there = lax.rem(here + i, n * groups)
        return pltpu.make_async_remote_copy(
            src_ref=sums.at[here],
            dst_ref=sums.at[here],
            send_sem=norm_send.at[i - 1],
            recv_sem=norm_recv.at[i - 1],
            device_id={"zero": there // groups, "cols": lax.rem(there, groups)},
            device_id_type=MESH,
        )

    def prepare(t, reused):
        slot, from_slot, a = lax.rem(t, SLOTS), lax.rem(t, 2), t // mains
        row = pl.multiple_of(first_row(z) + LANES * (t - a * mains), HALF)
        if reused:
            for j in range(1, n):
                bulk(t - SLOTS, j).wait_send()
        for j in range(n):
            load(0, 0, from_slot, j).wait()
            part = raw[from_slot, j].T
            if j:
                sent[slot, j - 1] = part
            else:
                final[a, pl.ds(row, LANES), lanes] = part

    def prepare_pair(a):
        for q in range(n // 2):
            load_pair(a, q).wait()
            sent_pair[a, q] = raw_pair[a, q].T
        own = sent_pair[a, z // 2, pl.ds(pl.multiple_of(first_row(z), HALF), HALF), :]
        final[a, pl.ds(pl.multiple_of(pair_row(z), HALF), HALF), lanes] = own

    def merge(a, row):
        row = pl.multiple_of(row, HALF)
        high = turned[a, pl.ds(pl.multiple_of(row + HALF * odd, HALF), HALF), :]
        size = None
        for s in range(n):
            cut = slice(s * rows, (s + 1) * rows)
            change = mix_rate * jnp.dot(high, lows[a, s], preferred_element_type=jnp.float32)
            part = final[a, pl.ds(row, HALF), cut].astype(jnp.float32) + change
            result[:, cut] = part
            here_size = jnp.sum(jnp.abs(part), axis=1, keepdims=True)
            size = here_size if size is None else size + here_size
        scale = size / (n * rows)
        scales[a, pl.ds(row, HALF), :] = scale
        inverse = 1.0 / scale
        for s in range(n):
            cut = slice(s * rows, (s + 1) * rows)
            final[a, pl.ds(row, HALF), cut] = (result[:, cut] * inverse).astype(final.dtype)

    def finish(t):
        for j in range(1, n):
            bulk(t, j).wait_recv()
        a = t // mains
        row = first_row(z) + LANES * (t - a * mains)
        lax.fori_loop(0, LANES // HALF, lambda i, c: (merge(a, row + HALF * i), c)[1], 0)

    def finish_pair(a):
        for j in range(1, n):
            pair(a, j).wait_recv()
        merge(a, pair_row(z))

    def send(t):
        for j in reversed(range(1, n)):
            bulk(t, j).start()

    def send_pair(a):
        for j in reversed(range(1, n)):
            pair(a, j).start()

    barrier = pltpu.get_barrier_semaphore()
    for i in range(1, n * groups):
        there = lax.rem(here + i, n * groups)
        pl.semaphore_signal(
            barrier, inc=1,
            device_id={"zero": there // groups, "cols": lax.rem(there, groups)},
            device_id_type=MESH,
        )
    for q in range(n // 2):
        load_pair(0, q).start()
    for a in range(2):
        pl.when(x == a)(lambda a=a: own_low(a).start())
    start_loads(0)
    start_loads(1)
    norm_loads = [
        pltpu.make_async_copy(norm_train, train, norm_sem.at[0]),
        pltpu.make_async_copy(norm_step, step, norm_sem.at[1]),
    ]
    for copy in norm_loads:
        copy.start()
    for a in range(2):
        own_high(a).start()
    for q in range(n // 2):
        load_pair(1, q).start()

    prepare_pair(0)
    for copy in norm_loads:
        copy.wait()
    sums[here] = train[...] + step[...]
    own_low(0).wait()
    pl.semaphore_wait(barrier, n * groups - 1)

    mate, inner = z + 1 - 2 * odd, (z == 1) | (z == 2)
    gateway, other = 2 - z // 2, 2 - 2 * (z // 2)
    low_copy(z, gateway, 0).start()
    low_copy(z, mate, 1).start()
    send_pair(0)
    prepare(0, False)
    start_loads(2)
    for i in range(1, n * groups):
        norm_copy(i).start()
    prepare(1, False)
    start_loads(3)
    send(0)

    @pl.when(inner)
    def _():
        for i in range(2):
            low_copy(other + i, mate, 2 + i).wait_recv()
            low_copy(other + i, mate, 2 + i).start()

    prepare(2, False)
    start_loads(4)
    send(1)
    for a in range(2):
        own_high(a).wait()
        turned[a] = highs[a].T
    prepare(3, False)
    start_loads(5)
    send(2)
    prepare_pair(1)

    low_copy(mate, mate, 0).wait_recv()

    @pl.when(jnp.logical_not(inner))
    def _():
        for i in range(2):
            low_copy(other + i, mate, 2 + i).wait_recv()

    low_swap().start()
    prepare(4, False)
    start_loads(6)
    send(3)
    low_swap().wait_recv()
    finish_pair(0)

    def at(k, carry):
        send(k + AHEAD)
        prepare(k + AHEAD + 1, True)

        @pl.when(k + AHEAD + 3 < steps)
        def _():
            start_loads(k + AHEAD + 3)

        finish(k)
        return carry

    send(4)
    prepare(5, False)
    start_loads(7)
    finish(0)
    lax.fori_loop(1, steps - AHEAD - 1, at, 0)
    send(steps - 1)
    send_pair(1)
    lax.fori_loop(steps - AHEAD - 1, steps, lambda k, c: (finish(k), c)[1], 0)

    for i in range(1, n * groups):
        norm_copy(i).wait_recv()
    for i in range(n * groups):
        length = sums.shape[2]
        norms[:, i * length : (i + 1) * length] = sums[i].astype(norms.dtype)
    finish_pair(1)

    for t in range(steps - SLOTS, steps):
        for j in range(1, n):
            bulk(t, j).wait_send()
    for a in range(2):
        for j in range(1, n):
            pair(a, j).wait_send()
    low_copy(z, gateway, 0).wait_send()
    low_copy(z, mate, 1).wait_send()

    @pl.when(inner)
    def _():
        for i in range(2):
            low_copy(other + i, mate, 2 + i).wait_send()

    low_swap().wait_send()
    for i in range(1, n * groups):
        norm_copy(i).wait_send()


def place_kernel(final, gate, up, sem):
    copies = [
        pltpu.make_async_copy(final.at[a], out, sem.at[a]) for a, out in enumerate((gate, up))
    ]
    for copy in copies:
        copy.start()
    for copy in copies:
        copy.wait()


def exchange(weight_gate, low_gate, high_gate, weight_up, low_up, high_up, norm_train, norm_step):
    n, groups = lax.axis_size("zero"), lax.axis_size("cols")
    rows, width = weight_gate.shape[0], weight_gate.shape[1] // n
    rank, length = low_gate.shape[1], norm_train.shape[0]
    steps = 2 * (width // LANES)
    dma = pltpu.SemaphoreType.DMA
    bf16, f32 = jnp.bfloat16, jnp.float32
    final, scales, norms = pl.pallas_call(
        functools.partial(exchange_kernel, n, groups),
        in_specs=[pl.BlockSpec(memory_space=pl.ANY)] * 8,
        out_specs=[pl.BlockSpec(memory_space=pltpu.VMEM)] * 3,
        out_shape=[
            pltpu.VMEM((2, width, n * rows), bf16),
            pltpu.VMEM((2, width, 1), f32),
            pltpu.VMEM((1, n * groups * length), bf16),
        ],
        scratch_shapes=[
            pltpu.VMEM((2, n, rows, LANES), bf16),
            pltpu.VMEM((2, n // 2, rows, LANES), bf16),
            pltpu.VMEM((SLOTS, n - 1, LANES, rows), bf16),
            pltpu.VMEM((2, n // 2, LANES, rows), bf16),
            pltpu.VMEM((2, n, rank, rows), bf16),
            pltpu.VMEM((2, rank, width + HALF), bf16),
            pltpu.VMEM((2, width + HALF, rank), bf16),
            pltpu.VMEM((HALF, n * rows), f32),
            pltpu.VMEM((1, length), f32),
            pltpu.VMEM((1, length), f32),
            pltpu.VMEM((n * groups, 1, length), f32),
            dma((2, n)),
            dma((2, n // 2)),
            dma,
            dma((2,)),
            dma((2,)),
            dma((SLOTS, n - 1)),
            dma((steps, n - 1)),
            dma((2, n - 1)),
            dma((2, n - 1)),
            dma((4,)),
            dma((n,)),
            dma((2,)),
            dma((n * groups - 1,)),
            dma((n * groups - 1,)),
        ],
        cost_estimate=pl.CostEstimate(
            flops=4 * width * n * rows * rank,
            bytes_accessed=8 * width * n * rows,
            transcendentals=0,
        ),
        compiler_params=pltpu.CompilerParams(
            collective_id=0, has_side_effects=True, vmem_limit_bytes=26 << 20
        ),
    )(
        weight_gate, weight_up, low_gate.T, low_up.T, high_gate, high_up,
        norm_train.reshape(1, length), norm_step.reshape(1, length),
    )
    gate, up = pl.pallas_call(
        place_kernel,
        in_specs=[pl.BlockSpec(memory_space=pltpu.VMEM)],
        out_specs=[pl.BlockSpec(memory_space=pl.ANY)] * 2,
        out_shape=[jax.ShapeDtypeStruct((width, n * rows), bf16)] * 2,
        scratch_shapes=[dma((2,))],
        compiler_params=pltpu.CompilerParams(vmem_limit_bytes=2 << 20),
    )(final)
    return gate.T, up.T, scales[0, :, 0], scales[1, :, 0], norms.reshape(-1)


def local(*args):
    n, groups = lax.axis_size("zero"), lax.axis_size("cols")
    rows, total = args[0].shape
    if n == 4 and groups == 2 and rows % LANES == 0 and (total // n) % LANES == HALF:
        return exchange(*args)
    return general(*args)


def solution(mesh):
    in_specs = (
        P(("unit", "zero"), "cols"),
        P(("unit", "zero"), None),
        P("unit", "cols"),
        P(("unit", "zero"), "cols"),
        P(("unit", "zero"), None),
        P("unit", "cols"),
        P(("unit", "zero", "cols")),
        P(("unit", "zero", "cols")),
    )
    out_specs = (
        P("unit", ("cols", "zero")),
        P("unit", ("cols", "zero")),
        P(("unit", "cols", "zero")),
        P(("unit", "cols", "zero")),
        P("unit"),
    )
    return jax.shard_map(local, mesh=mesh, in_specs=in_specs, out_specs=out_specs, check_vma=False)
```

```python
import functools

import jax
import jax.numpy as jnp
from jax import lax
from jax.experimental import pallas as pl
from jax.experimental.pallas import tpu as pltpu
from jax.sharding import PartitionSpec as P

mix_rate = 0.5


def cuts(units, shares):
    total, marks, seen = sum(shares), [0], 0
    for share in shares:
        seen += share
        marks.append(units * seen // total)
    return [(a, b) for a, b in zip(marks[:-1], marks[1:]) if b > a]


def merge_kernel(block_ref, low_ref, high_ref, *refs):
    final_ref, scale_ref, result_ref = refs[-3:]
    n, _, rows = block_ref.shape
    change = mix_rate * jnp.dot(high_ref[...], low_ref[...], preferred_element_type=jnp.float32)
    total = None
    for s in range(n):
        part = block_ref[s].astype(jnp.float32) + change[:, s * rows : (s + 1) * rows]
        result_ref[:, s * rows : (s + 1) * rows] = part
        size = jnp.sum(jnp.abs(part), axis=1, keepdims=True)
        total = size if total is None else total + size
    scale = total / (n * rows)
    scale_ref[...] = scale
    final_ref[...] = (result_ref[...] / scale).astype(final_ref.dtype)


def merge(block, low, high, final, first, step, width):
    n, part, rows = block.shape
    rank = low.shape[0]
    offset = first // step
    operands = [block, low, high]
    in_specs = [
        pl.BlockSpec((n, step, rows), lambda i: (0, i, 0)),
        pl.BlockSpec((rank, n * rows), lambda i: (0, 0)),
        pl.BlockSpec((step, rank), lambda i: (i + offset, 0)),
    ]
    aliases = {}
    if final is not None:
        operands.append(final)
        in_specs.append(pl.BlockSpec(memory_space=pl.ANY))
        aliases = {3: 0}
    return pl.pallas_call(
        merge_kernel,
        grid=(part // step,),
        in_specs=in_specs,
        out_specs=[
            pl.BlockSpec((step, n * rows), lambda i: (i + offset, 0)),
            pl.BlockSpec((step, 1), lambda i: (i, 0)),
        ],
        out_shape=[
            jax.ShapeDtypeStruct((width, n * rows), jnp.bfloat16),
            jax.ShapeDtypeStruct((part, 1), jnp.float32),
        ],
        scratch_shapes=[pltpu.VMEM((step, n * rows), jnp.float32)],
        input_output_aliases=aliases,
        cost_estimate=pl.CostEstimate(
            flops=2 * part * n * rows * rank,
            bytes_accessed=4 * part * n * rows,
            transcendentals=0,
        ),
        compiler_params=pltpu.CompilerParams(vmem_limit_bytes=24 << 20),
    )(*operands)


def general(weight_gate, low_gate, high_gate, weight_up, low_up, high_up, norm_train, norm_step):
    n = lax.axis_size("zero")
    rows, width = weight_gate.shape[0], weight_gate.shape[1] // n
    rank = low_gate.shape[1]
    place = lax.axis_index("zero")
    step = next(s for s in (48, 24, 16, 8, width) if width % s == 0)

    lows = lax.all_gather(
        jnp.concatenate([low_gate.T, low_up.T], axis=0), "zero", axis=1, tiled=True
    )
    serve_norm = lax.all_gather(
        (norm_train + norm_step).astype(jnp.bfloat16), ("zero", "cols"), axis=0, tiled=True
    )
    lows, serve_norm, weight_gate, weight_up = lax.optimization_barrier(
        (lows, serve_norm, weight_gate, weight_up)
    )
    low = {"gate": lows[:rank], "up": lows[rank:]}
    high = {
        "gate": lax.dynamic_slice_in_dim(high_gate, place * width, width, axis=1).T,
        "up": lax.dynamic_slice_in_dim(high_up, place * width, width, axis=1).T,
    }
    turned = {
        "gate": weight_gate.T.reshape(n, width, rows),
        "up": weight_up.T.reshape(n, width, rows),
    }

    shares = {"gate": (1, 3), "up": (7, 2)}
    jobs = [
        (name, a * step, b * step)
        for name in ("gate", "up")
        for a, b in cuts(width // step, shares[name])
    ]
    finals = {"gate": None, "up": None}
    scales = {"gate": [], "up": []}
    block = None
    arrived = []
    for name, a, b in jobs:
        sent = turned[name][:, a:b]
        if block is not None:
            sent, block = lax.optimization_barrier((sent, block))
            arrived.append(block)
        block = lax.all_to_all(sent, "zero", split_axis=0, concat_axis=0, tiled=True)
    arrived.append(block)
    for (name, a, b), block in zip(jobs, arrived):
        finals[name], scale = merge(block, low[name], high[name], finals[name], a, step, width)
        scales[name].append(scale[:, 0])
    return (
        finals["gate"].T,
        finals["up"].T,
        jnp.concatenate(scales["gate"]),
        jnp.concatenate(scales["up"]),
        serve_norm,
    )


MESH = pl.DeviceIdType.MESH
LANES, HALF, LAST, AHEAD, PIECES = 128, 64, 32, 4, 4
SLOTS = AHEAD + 2


def peer(z, n, shift):
    return lax.rem(z + shift, n)


def first_row(d):
    return HALF * lax.rem(d, 2)


def pair_row(d, width):
    return pl.multiple_of((width - HALF) * (1 - lax.rem(d, 2)), HALF)


def enter(places):
    barrier = pltpu.get_barrier_semaphore()
    for place in places:
        pl.semaphore_signal(barrier, inc=1, device_id=place, device_id_type=MESH)
    return lambda: pl.semaphore_wait(barrier, len(places))


def exchange_kernel(
    n, groups,
    weight_gate, weight_up, low_gate, low_up, high_gate, high_up, norm_train, norm_step,
    final, scales, sums,
    raw, raw_pair, sent, sent_pair, lows, highs, turned, result, train, step,
    raw_sem, pair_sem, low_sem, high_sem, norm_sem,
    send_sem, recv_sem, pair_send, pair_recv, low_send, low_recv, swap_sem, norm_send, norm_recv,
):
    rows, total = weight_gate.shape
    width = total // n
    mains = width // LANES
    steps = 2 * mains
    weights, own_lows, own_highs = (weight_gate, weight_up), (low_gate, low_up), (high_gate, high_up)
    z, x = lax.axis_index("zero"), lax.axis_index("cols")
    odd = lax.rem(z, 2)
    here = z * groups + x
    lanes = pl.ds(pl.multiple_of(z * rows, LANES), rows)

    def place(i):
        there = lax.rem(here + i, n * groups)
        return {"zero": there // groups, "cols": lax.rem(there, groups)}

    def load(a, s, slot, j):
        d = peer(z, n, j)
        tile = (d // 2) * (2 * width // LANES) + lax.rem(d, 2) * (mains + 1) + s
        start = pl.multiple_of(tile * LANES, LANES)
        return pltpu.make_async_copy(
            weights[a].at[:, pl.ds(start, LANES)], raw.at[slot, j], raw_sem.at[slot, j]
        )

    def start_loads(t):
        def go(a):
            for j in reversed(range(n)):
                load(a, t - a * mains, lax.rem(t, 2), j).start()

        if isinstance(t, int):
            go(t // mains)
        else:
            for a in range(2):
                pl.when(t // mains == a)(functools.partial(go, a))

    def load_pair(a, q):
        tile = q * (2 * width // LANES) + mains
        return pltpu.make_async_copy(
            weights[a].at[:, pl.ds(tile * LANES, LANES)], raw_pair.at[a, q], pair_sem.at[a, q]
        )

    def own_low(a):
        return pltpu.make_async_copy(own_lows[a], lows.at[a, z], low_sem)

    def own_high(a):
        start = pl.multiple_of(z * width - HALF * odd, LANES)
        return pltpu.make_async_copy(
            own_highs[a].at[:, pl.ds(start, width + HALF)], highs.at[a], high_sem.at[a]
        )

    def bulk(t, j):
        d = peer(z, n, j)
        a = t // mains
        row = pl.multiple_of(first_row(d) + LANES * (t - a * mains), HALF)
        slot = lax.rem(t, SLOTS)
        return pltpu.make_async_remote_copy(
            src_ref=sent.at[slot, j - 1],
            dst_ref=final.at[a, pl.ds(row, LANES), lanes],
            send_sem=send_sem.at[slot, j - 1],
            recv_sem=recv_sem.at[t, j - 1],
            device_id={"zero": d},
            device_id_type=MESH,
        )

    def pair(a, j, cut=0, height=HALF):
        d = peer(z, n, j)
        source = pl.multiple_of(first_row(d) + cut, height)
        target = pl.multiple_of(pair_row(d, width) + cut, height)
        index = a + cut // height
        return pltpu.make_async_remote_copy(
            src_ref=sent_pair.at[a, d // 2, pl.ds(source, height)],
            dst_ref=final.at[a, pl.ds(target, height), lanes],
            send_sem=pair_send.at[index, j - 1],
            recv_sem=pair_recv.at[index, j - 1],
            device_id={"zero": d},
            device_id_type=MESH,
        )

    def low_copy(block, d, index):
        return pltpu.make_async_remote_copy(
            src_ref=lows.at[x, block],
            dst_ref=lows.at[x, block],
            send_sem=low_send.at[index],
            recv_sem=low_recv.at[block],
            device_id={"zero": d},
            device_id_type=MESH,
        )

    def low_swap():
        return pltpu.make_async_remote_copy(
            src_ref=lows.at[x],
            dst_ref=lows.at[x],
            send_sem=swap_sem.at[0],
            recv_sem=swap_sem.at[1],
            device_id={"cols": 1 - x},
            device_id_type=MESH,
        )

    def norm_copy(i):
        return pltpu.make_async_remote_copy(
            src_ref=sums.at[here],
            dst_ref=sums.at[here],
            send_sem=norm_send.at[i - 1],
            recv_sem=norm_recv.at[i - 1],
            device_id=place(i),
            device_id_type=MESH,
        )

    def prepare(t, reused):
        slot, from_slot, a = lax.rem(t, SLOTS), lax.rem(t, 2), t // mains
        if reused:
            for j in range(1, n):
                bulk(t - SLOTS, j).wait_send()
        for j in reversed(range(n)):
            load(0, 0, from_slot, j).wait()
            part = raw[from_slot, j].T
            if j:
                sent[slot, j - 1] = part
            else:
                row = pl.multiple_of(first_row(z) + LANES * (t - a * mains), HALF)
                final[a, pl.ds(row, LANES), lanes] = part

    def prepare_pair(a):
        for q in range(n // 2):
            load_pair(a, q).wait()
            sent_pair[a, q] = raw_pair[a, q].T

    def keep_pair(a):
        own = sent_pair[a, z // 2, pl.ds(pl.multiple_of(first_row(z), HALF), HALF), :]
        final[a, pl.ds(pair_row(z, width), HALF), lanes] = own

    def merge(a, row, height):
        row = pl.multiple_of(row, height)
        span = pl.ds(row, height)
        high = turned[a, pl.ds(pl.multiple_of(row + HALF * odd, height), height), :]
        size = None
        for s in range(n):
            cut = slice(s * rows, (s + 1) * rows)
            change = mix_rate * jnp.dot(high, lows[a, s], preferred_element_type=jnp.float32)
            part = final[a, span, cut].astype(jnp.float32) + change
            result[:height, cut] = part
            mine = jnp.sum(jnp.abs(part), axis=1, keepdims=True)
            size = mine if size is None else size + mine
        scale = size / (n * rows)
        scales[a, span, :] = scale
        inverse = 1.0 / scale
        for s in range(n):
            cut = slice(s * rows, (s + 1) * rows)
            final[a, span, cut] = (result[:height, cut] * inverse).astype(final.dtype)

    def finish(t):
        for j in range(1, n):
            bulk(t, j).wait_recv()
        a = t // mains
        row = first_row(z) + LANES * (t - a * mains)
        lax.fori_loop(0, LANES // HALF, lambda i, c: (merge(a, row + HALF * i, HALF), c)[1], 0)

    def send(t):
        for j in reversed(range(1, n)):
            bulk(t, j).start()

    wait_for_all = enter([place(i) for i in range(1, n * groups)])
    for a in range(2):
        pl.when(x == a)(lambda a=a: own_low(a).start())
    for q in range(n // 2):
        load_pair(0, q).start()
    start_loads(0)
    start_loads(1)
    norm_loads = [
        pltpu.make_async_copy(norm_train, train, norm_sem.at[0]),
        pltpu.make_async_copy(norm_step, step, norm_sem.at[1]),
    ]
    for copy in norm_loads:
        copy.start()
    for a in range(2):
        own_high(a).start()
    for q in range(n // 2):
        load_pair(1, q).start()

    mate, inner = z + 1 - 2 * odd, (z == 1) | (z == 2)
    gateway, other = 2 - z // 2, 2 - 2 * (z // 2)
    own_low(0).wait()
    prepare_pair(0)
    wait_for_all()
    low_copy(z, gateway, 0).start()
    low_copy(z, mate, 1).start()
    for copy in norm_loads:
        copy.wait()
    sums[here] = (train[...] + step[...]).reshape(1, -1)
    for j in reversed(range(1, n)):
        pair(0, j).start()
    keep_pair(0)
    prepare(0, False)
    start_loads(2)
    for i in range(1, n * groups):
        norm_copy(i).start()
    prepare(1, False)
    start_loads(3)
    send(0)

    @pl.when(inner)
    def _():
        for i in range(2):
            low_copy(other + i, mate, 2 + i).wait_recv()
            low_copy(other + i, mate, 2 + i).start()

    t = 2
    while t < AHEAD + 1:
        prepare(t, False)
        start_loads(t + 2)
        send(t - 1)
        t += 1
    for a in range(2):
        own_high(a).wait()
        turned[a] = highs[a].T
    prepare_pair(1)
    keep_pair(1)

    low_copy(mate, mate, 0).wait_recv()

    @pl.when(jnp.logical_not(inner))
    def _():
        for i in range(2):
            low_copy(other + i, mate, 2 + i).wait_recv()

    low_swap().start()
    low_swap().wait_recv()
    for j in range(1, n):
        pair(0, j).wait_recv()
    merge(0, pair_row(z, width), HALF)

    send(AHEAD)
    prepare(AHEAD + 1, False)
    start_loads(AHEAD + 3)
    finish(0)

    def at(k, carry):
        send(k + AHEAD)
        prepare(k + AHEAD + 1, True)

        @pl.when(k + AHEAD + 3 < steps)
        def _():
            start_loads(k + AHEAD + 3)

        finish(k)
        return carry

    lax.fori_loop(1, steps - AHEAD - 1, at, 0)
    send(steps - 1)
    for part in range(2):
        for j in reversed(range(1, n)):
            pair(1, j, part * LAST, LAST).start()
    for i in range(1, n * groups):
        norm_copy(i).wait_recv()
    lax.fori_loop(steps - AHEAD - 1, steps, lambda k, c: (finish(k), c)[1], 0)

    for t in range(steps - SLOTS, steps):
        for j in range(1, n):
            bulk(t, j).wait_send()
    for j in range(1, n):
        pair(0, j).wait_send()
    low_copy(z, gateway, 0).wait_send()
    low_copy(z, mate, 1).wait_send()

    @pl.when(inner)
    def _():
        for i in range(2):
            low_copy(other + i, mate, 2 + i).wait_send()

    low_swap().wait_send()
    for i in range(1, n * groups):
        norm_copy(i).wait_send()
    for part in range(2):
        for j in range(1, n):
            pair(1, j, part * LAST, LAST).wait_recv()
        merge(1, pair_row(z, width) + part * LAST, LAST)
    for part in range(2):
        for j in range(1, n):
            pair(1, j, part * LAST, LAST).wait_send()


def to_lanes(column):
    n = column.shape[0]
    if n < LANES:
        column = jnp.concatenate([column, jnp.zeros((LANES - n, 1), column.dtype)], axis=0)
    return jnp.broadcast_to(column, (LANES, LANES)).T[0, :n]


def place_kernel(final, scales, sums, gate, up, scale_gate, scale_up, norm, sem):
    width = scale_gate.shape[0]
    copies = [
        pltpu.make_async_copy(
            final.at[a, pl.ds(i * width // PIECES, width // PIECES)],
            out.at[pl.ds(i * width // PIECES, width // PIECES)],
            sem.at[a, i],
        )
        for i in range(PIECES)
        for a, out in enumerate((gate, up))
    ]
    for copy in copies:
        copy.start()
    for a, out in enumerate((scale_gate, scale_up)):
        for k in range(0, width, LANES):
            w = min(LANES, width - k)
            out[pl.ds(k, w)] = to_lanes(scales[a, pl.ds(k, w), :])
    length = sums.shape[2]
    for i in range(sums.shape[0]):
        norm[pl.ds(i * length, length)] = sums[i, 0].astype(norm.dtype)
    for copy in copies:
        copy.wait()


def exchange(weight_gate, low_gate, high_gate, weight_up, low_up, high_up, norm_train, norm_step):
    n, groups = lax.axis_size("zero"), lax.axis_size("cols")
    rows, width = weight_gate.shape[0], weight_gate.shape[1] // n
    rank, length = low_gate.shape[1], norm_train.shape[0]
    steps = 2 * (width // LANES)
    dma = pltpu.SemaphoreType.DMA
    bf16, f32 = jnp.bfloat16, jnp.float32
    vmem, hbm = pl.BlockSpec(memory_space=pltpu.VMEM), pl.BlockSpec(memory_space=pl.ANY)
    final, scales, sums = pl.pallas_call(
        functools.partial(exchange_kernel, n, groups),
        in_specs=[hbm] * 8,
        out_specs=[vmem] * 3,
        out_shape=[
            pltpu.VMEM((2, width, n * rows), bf16),
            pltpu.VMEM((2, width, 1), f32),
            pltpu.VMEM((n * groups, 1, length), f32),
        ],
        scratch_shapes=[
            pltpu.VMEM((2, n, rows, LANES), bf16),
            pltpu.VMEM((2, n // 2, rows, LANES), bf16),
            pltpu.VMEM((SLOTS, n - 1, LANES, rows), bf16),
            pltpu.VMEM((2, n // 2, LANES, rows), bf16),
            pltpu.VMEM((2, n, rank, rows), bf16),
            pltpu.VMEM((2, rank, width + HALF), bf16),
            pltpu.VMEM((2, width + HALF, rank), bf16),
            pltpu.VMEM((HALF, n * rows), f32),
            pltpu.VMEM((length,), f32),
            pltpu.VMEM((length,), f32),
            dma((2, n)),
            dma((2, n // 2)),
            dma,
            dma((2,)),
            dma((2,)),
            dma((SLOTS, n - 1)),
            dma((steps, n - 1)),
            dma((3, n - 1)),
            dma((3, n - 1)),
            dma((4,)),
            dma((n,)),
            dma((2,)),
            dma((n * groups - 1,)),
            dma((n * groups - 1,)),
        ],
        cost_estimate=pl.CostEstimate(
            flops=4 * width * n * rows * rank,
            bytes_accessed=8 * width * n * rows,
            transcendentals=0,
        ),
        compiler_params=pltpu.CompilerParams(
            collective_id=0, has_side_effects=True, vmem_limit_bytes=24 << 20
        ),
    )(weight_gate, weight_up, low_gate.T, low_up.T, high_gate, high_up, norm_train, norm_step)
    gate, up, scale_gate, scale_up, norm = pl.pallas_call(
        place_kernel,
        in_specs=[vmem] * 3,
        out_specs=[hbm] * 2 + [vmem] * 3,
        out_shape=[
            jax.ShapeDtypeStruct((width, n * rows), bf16),
            jax.ShapeDtypeStruct((width, n * rows), bf16),
            jax.ShapeDtypeStruct((width,), f32),
            jax.ShapeDtypeStruct((width,), f32),
            jax.ShapeDtypeStruct((n * groups * length,), bf16),
        ],
        scratch_shapes=[dma((2, PIECES))],
        compiler_params=pltpu.CompilerParams(vmem_limit_bytes=24 << 20),
    )(*(pltpu.with_memory_space_constraint(v, pltpu.VMEM) for v in (final, scales, sums)))
    return gate.T, up.T, scale_gate, scale_up, norm


def local(*args):
    n, groups = lax.axis_size("zero"), lax.axis_size("cols")
    rows, total = args[0].shape
    if n == 4 and groups == 2 and rows % LANES == 0 and (total // n) % LANES == HALF:
        return exchange(*args)
    return general(*args)


def solution(mesh):
    in_specs = (
        P(("unit", "zero"), "cols"),
        P(("unit", "zero"), None),
        P("unit", "cols"),
        P(("unit", "zero"), "cols"),
        P(("unit", "zero"), None),
        P("unit", "cols"),
        P(("unit", "zero", "cols")),
        P(("unit", "zero", "cols")),
    )
    out_specs = (
        P("unit", ("cols", "zero")),
        P("unit", ("cols", "zero")),
        P(("unit", "cols", "zero")),
        P(("unit", "cols", "zero")),
        P("unit"),
    )
    return jax.shard_map(local, mesh=mesh, in_specs=in_specs, out_specs=out_specs, check_vma=False)
```

```python
import functools

import jax
import jax.numpy as jnp
from jax import lax
from jax.experimental import pallas as pl
from jax.experimental.pallas import tpu as pltpu
from jax.sharding import PartitionSpec as P

mix_rate = 0.5


def cuts(units, shares):
    total, marks, seen = sum(shares), [0], 0
    for share in shares:
        seen += share
        marks.append(units * seen // total)
    return [(a, b) for a, b in zip(marks[:-1], marks[1:]) if b > a]


def merge_kernel(block_ref, low_ref, high_ref, *refs):
    final_ref, scale_ref, result_ref = refs[-3:]
    n, _, rows = block_ref.shape
    change = mix_rate * jnp.dot(high_ref[...], low_ref[...], preferred_element_type=jnp.float32)
    total = None
    for s in range(n):
        part = block_ref[s].astype(jnp.float32) + change[:, s * rows : (s + 1) * rows]
        result_ref[:, s * rows : (s + 1) * rows] = part
        size = jnp.sum(jnp.abs(part), axis=1, keepdims=True)
        total = size if total is None else total + size
    scale = total / (n * rows)
    scale_ref[...] = scale
    final_ref[...] = (result_ref[...] / scale).astype(final_ref.dtype)


def merge(block, low, high, final, first, step, width):
    n, part, rows = block.shape
    rank = low.shape[0]
    offset = first // step
    operands = [block, low, high]
    in_specs = [
        pl.BlockSpec((n, step, rows), lambda i: (0, i, 0)),
        pl.BlockSpec((rank, n * rows), lambda i: (0, 0)),
        pl.BlockSpec((step, rank), lambda i: (i + offset, 0)),
    ]
    aliases = {}
    if final is not None:
        operands.append(final)
        in_specs.append(pl.BlockSpec(memory_space=pl.ANY))
        aliases = {3: 0}
    return pl.pallas_call(
        merge_kernel,
        grid=(part // step,),
        in_specs=in_specs,
        out_specs=[
            pl.BlockSpec((step, n * rows), lambda i: (i + offset, 0)),
            pl.BlockSpec((step, 1), lambda i: (i, 0)),
        ],
        out_shape=[
            jax.ShapeDtypeStruct((width, n * rows), jnp.bfloat16),
            jax.ShapeDtypeStruct((part, 1), jnp.float32),
        ],
        scratch_shapes=[pltpu.VMEM((step, n * rows), jnp.float32)],
        input_output_aliases=aliases,
        cost_estimate=pl.CostEstimate(
            flops=2 * part * n * rows * rank,
            bytes_accessed=4 * part * n * rows,
            transcendentals=0,
        ),
        compiler_params=pltpu.CompilerParams(vmem_limit_bytes=24 << 20),
    )(*operands)


def general(weight_gate, low_gate, high_gate, weight_up, low_up, high_up, norm_train, norm_step):
    n = lax.axis_size("zero")
    rows, width = weight_gate.shape[0], weight_gate.shape[1] // n
    rank = low_gate.shape[1]
    place = lax.axis_index("zero")
    step = next(s for s in (48, 24, 16, 8, width) if width % s == 0)

    lows = lax.all_gather(
        jnp.concatenate([low_gate.T, low_up.T], axis=0), "zero", axis=1, tiled=True
    )
    serve_norm = lax.all_gather(
        (norm_train + norm_step).astype(jnp.bfloat16), ("zero", "cols"), axis=0, tiled=True
    )
    lows, serve_norm, weight_gate, weight_up = lax.optimization_barrier(
        (lows, serve_norm, weight_gate, weight_up)
    )
    low = {"gate": lows[:rank], "up": lows[rank:]}
    high = {
        "gate": lax.dynamic_slice_in_dim(high_gate, place * width, width, axis=1).T,
        "up": lax.dynamic_slice_in_dim(high_up, place * width, width, axis=1).T,
    }
    turned = {
        "gate": weight_gate.T.reshape(n, width, rows),
        "up": weight_up.T.reshape(n, width, rows),
    }

    shares = {"gate": (1, 3), "up": (7, 2)}
    jobs = [
        (name, a * step, b * step)
        for name in ("gate", "up")
        for a, b in cuts(width // step, shares[name])
    ]
    finals = {"gate": None, "up": None}
    scales = {"gate": [], "up": []}
    block = None
    arrived = []
    for name, a, b in jobs:
        sent = turned[name][:, a:b]
        if block is not None:
            sent, block = lax.optimization_barrier((sent, block))
            arrived.append(block)
        block = lax.all_to_all(sent, "zero", split_axis=0, concat_axis=0, tiled=True)
    arrived.append(block)
    for (name, a, b), block in zip(jobs, arrived):
        finals[name], scale = merge(block, low[name], high[name], finals[name], a, step, width)
        scales[name].append(scale[:, 0])
    return (
        finals["gate"].T,
        finals["up"].T,
        jnp.concatenate(scales["gate"]),
        jnp.concatenate(scales["up"]),
        serve_norm,
    )


MESH = pl.DeviceIdType.MESH
LANES, HALF, AHEAD, PIECES, GRANT = 128, 64, 4, 4, 22 << 20
SLOTS = AHEAD + 2


def peer(z, n, shift):
    return lax.rem(z + shift, n)


def first_row(d):
    return HALF * lax.rem(d, 2)


def pair_row(d, width):
    return pl.multiple_of((width - HALF) * (1 - lax.rem(d, 2)), HALF)


def enter(places):
    barrier = pltpu.get_barrier_semaphore()
    for place in places:
        pl.semaphore_signal(barrier, inc=1, device_id=place, device_id_type=MESH)
    return lambda: pl.semaphore_wait(barrier, len(places))


def combine(source, row, high, lows, result, target, place):
    n, _, rows = lows.shape
    span = pl.ds(row, HALF)
    size = None
    for s in range(n):
        cut = slice(s * rows, (s + 1) * rows)
        change = mix_rate * jnp.dot(high, lows[s], preferred_element_type=jnp.float32)
        part = source[span, cut].astype(jnp.float32) + change
        result[:, cut] = part
        mine = jnp.sum(jnp.abs(part), axis=1, keepdims=True)
        size = mine if size is None else size + mine
    scale = size / (n * rows)
    inverse = 1.0 / scale
    for s in range(n):
        cut = slice(s * rows, (s + 1) * rows)
        target[pl.ds(place, HALF), cut] = (result[:, cut] * inverse).astype(target.dtype)
    return scale


def exchange_kernel(
    n, groups,
    weight_gate, weight_up, low_gate, low_up, high_gate, high_up, norm_train, norm_step,
    final, scales, sums, lows, turned, piece_0, piece_1, piece_2, piece_3,
    raw, raw_pair, sent, sent_pair, highs, result, train, step,
    raw_sem, pair_sem, low_sem, high_sem, norm_sem,
    send_sem, recv_sem, pair_send, pair_recv, low_send, low_recv, swap_sem, norm_send, norm_recv,
    piece_sem,
):
    rows, total = weight_gate.shape
    width = total // n
    mains = width // LANES
    steps = 2 * mains
    weights, own_lows, own_highs = (weight_gate, weight_up), (low_gate, low_up), (high_gate, high_up)
    z, x = lax.axis_index("zero"), lax.axis_index("cols")
    odd = lax.rem(z, 2)
    here = z * groups + x
    lanes = pl.ds(pl.multiple_of(z * rows, LANES), rows)

    def place(i):
        there = lax.rem(here + i, n * groups)
        return {"zero": there // groups, "cols": lax.rem(there, groups)}

    def load(a, s, slot, j):
        d = peer(z, n, j)
        tile = (d // 2) * (2 * width // LANES) + lax.rem(d, 2) * (mains + 1) + s
        start = pl.multiple_of(tile * LANES, LANES)
        return pltpu.make_async_copy(
            weights[a].at[:, pl.ds(start, LANES)], raw.at[slot, j], raw_sem.at[slot, j]
        )

    def start_loads(t):
        def go(a):
            for j in reversed(range(n)):
                load(a, t - a * mains, lax.rem(t, 2), j).start()

        if isinstance(t, int):
            go(t // mains)
        else:
            for a in range(2):
                pl.when(t // mains == a)(functools.partial(go, a))

    def load_pair(a, q):
        tile = q * (2 * width // LANES) + mains
        return pltpu.make_async_copy(
            weights[a].at[:, pl.ds(tile * LANES, LANES)], raw_pair.at[a, q], pair_sem.at[a, q]
        )

    def own_low(a):
        return pltpu.make_async_copy(own_lows[a], lows.at[a, z], low_sem)

    def own_high(a):
        start = pl.multiple_of(z * width - HALF * odd, LANES)
        return pltpu.make_async_copy(
            own_highs[a].at[:, pl.ds(start, width + HALF)], highs.at[a], high_sem.at[a]
        )

    def bulk(t, j):
        d = peer(z, n, j)
        a = t // mains
        row = pl.multiple_of(first_row(d) + LANES * (t - a * mains), HALF)
        slot = lax.rem(t, SLOTS)
        return pltpu.make_async_remote_copy(
            src_ref=sent.at[slot, j - 1],
            dst_ref=final.at[a, pl.ds(row, LANES), lanes],
            send_sem=send_sem.at[slot, j - 1],
            recv_sem=recv_sem.at[t, j - 1],
            device_id={"zero": d},
            device_id_type=MESH,
        )

    def pair_of(a, d):
        return sent_pair.at[a, d // 2, pl.ds(pl.multiple_of(first_row(d), HALF), HALF)]

    def pair(j):
        d = peer(z, n, j)
        return pltpu.make_async_remote_copy(
            src_ref=pair_of(0, d),
            dst_ref=final.at[0, pl.ds(pair_row(d, width), HALF), lanes],
            send_sem=pair_send.at[j - 1],
            recv_sem=pair_recv.at[j - 1],
            device_id={"zero": d},
            device_id_type=MESH,
        )

    def piece_copy(j):
        out = (piece_0, piece_1, piece_2, piece_3)[j]
        return pltpu.make_async_copy(pair_of(1, peer(z, n, j)), out, piece_sem.at[j])

    def low_copy(block, d, index):
        return pltpu.make_async_remote_copy(
            src_ref=lows.at[x, block],
            dst_ref=lows.at[x, block],
            send_sem=low_send.at[index],
            recv_sem=low_recv.at[block],
            device_id={"zero": d},
            device_id_type=MESH,
        )

    def low_swap():
        return pltpu.make_async_remote_copy(
            src_ref=lows.at[x],
            dst_ref=lows.at[x],
            send_sem=swap_sem.at[0],
            recv_sem=swap_sem.at[1],
            device_id={"cols": 1 - x},
            device_id_type=MESH,
        )

    def norm_copy(i):
        return pltpu.make_async_remote_copy(
            src_ref=sums.at[here],
            dst_ref=sums.at[here],
            send_sem=norm_send.at[i - 1],
            recv_sem=norm_recv.at[i - 1],
            device_id=place(i),
            device_id_type=MESH,
        )

    def prepare(t, reused):
        slot, from_slot, a = lax.rem(t, SLOTS), lax.rem(t, 2), t // mains
        if reused:
            for j in range(1, n):
                bulk(t - SLOTS, j).wait_send()
        for j in reversed(range(n)):
            load(0, 0, from_slot, j).wait()
            part = raw[from_slot, j].T
            if j:
                sent[slot, j - 1] = part
            else:
                row = pl.multiple_of(first_row(z) + LANES * (t - a * mains), HALF)
                final[a, pl.ds(row, LANES), lanes] = part

    def prepare_pair(a):
        for q in range(n // 2):
            load_pair(a, q).wait()
            sent_pair[a, q] = raw_pair[a, q].T

    def keep_pair(a):
        own = sent_pair[a, z // 2, pl.ds(pl.multiple_of(first_row(z), HALF), HALF), :]
        final[a, pl.ds(pair_row(z, width), HALF), lanes] = own

    def merge_at(a, row):
        row = pl.multiple_of(row, HALF)
        high = turned[a, pl.ds(pl.multiple_of(row + HALF * odd, HALF), HALF), :]
        scale = combine(final.at[a], row, high, lows.at[a], result, final.at[a], row)
        scales[a, pl.ds(row, HALF), :] = scale

    def finish(t):
        for j in range(1, n):
            bulk(t, j).wait_recv()
        a = t // mains
        row = first_row(z) + LANES * (t - a * mains)
        lax.fori_loop(0, LANES // HALF, lambda i, c: (merge_at(a, row + HALF * i), c)[1], 0)

    def send(t):
        for j in reversed(range(1, n)):
            bulk(t, j).start()

    wait_for_all = enter([place(i) for i in range(1, n * groups)])
    for a in range(2):
        pl.when(x == a)(lambda a=a: own_low(a).start())
    for q in range(n // 2):
        load_pair(0, q).start()
    start_loads(0)
    start_loads(1)
    norm_loads = [
        pltpu.make_async_copy(norm_train, train, norm_sem.at[0]),
        pltpu.make_async_copy(norm_step, step, norm_sem.at[1]),
    ]
    for copy in norm_loads:
        copy.start()
    for a in range(2):
        own_high(a).start()
    for q in range(n // 2):
        load_pair(1, q).start()

    mate, inner = z + 1 - 2 * odd, (z == 1) | (z == 2)
    gateway, other = 2 - z // 2, 2 - 2 * (z // 2)
    own_low(0).wait()
    prepare_pair(0)
    wait_for_all()
    low_copy(z, gateway, 0).start()
    low_copy(z, mate, 1).start()
    for copy in norm_loads:
        copy.wait()
    sums[here] = (train[...] + step[...]).reshape(1, -1)
    for j in reversed(range(1, n)):
        pair(j).start()
    keep_pair(0)
    prepare(0, False)
    start_loads(2)
    for i in range(1, n * groups):
        norm_copy(i).start()
    prepare(1, False)
    start_loads(3)
    send(0)

    @pl.when(inner)
    def _():
        for i in range(2):
            low_copy(other + i, mate, 2 + i).wait_recv()
            low_copy(other + i, mate, 2 + i).start()

    t = 2
    while t < AHEAD + 1:
        prepare(t, False)
        start_loads(t + 2)
        send(t - 1)
        t += 1
    for a in range(2):
        own_high(a).wait()
        turned[a] = highs[a].T
    prepare_pair(1)

    low_copy(mate, mate, 0).wait_recv()

    @pl.when(jnp.logical_not(inner))
    def _():
        for i in range(2):
            low_copy(other + i, mate, 2 + i).wait_recv()

    low_swap().start()
    low_swap().wait_recv()
    for j in range(n):
        piece_copy(j).start()
    for j in range(1, n):
        pair(j).wait_recv()
    merge_at(0, pair_row(z, width))

    send(AHEAD)
    prepare(AHEAD + 1, False)
    start_loads(AHEAD + 3)
    finish(0)

    def at(k, carry):
        send(k + AHEAD)
        prepare(k + AHEAD + 1, True)

        @pl.when(k + AHEAD + 3 < steps)
        def _():
            start_loads(k + AHEAD + 3)

        finish(k)
        return carry

    lax.fori_loop(1, steps - AHEAD - 1, at, 0)
    send(steps - 1)
    for j in range(n):
        piece_copy(j).wait()
    for i in range(1, n * groups):
        norm_copy(i).wait_recv()
    lax.fori_loop(steps - AHEAD - 1, steps - 1, lambda k, c: (finish(k), c)[1], 0)
    for j in range(1, n):
        bulk(steps - 1, j).wait_recv()

    for t in range(steps - SLOTS, steps):
        for j in range(1, n):
            bulk(t, j).wait_send()
    for j in range(1, n):
        pair(j).wait_send()
    low_copy(z, gateway, 0).wait_send()
    low_copy(z, mate, 1).wait_send()

    @pl.when(inner)
    def _():
        for i in range(2):
            low_copy(other + i, mate, 2 + i).wait_send()

    low_swap().wait_send()
    for i in range(1, n * groups):
        norm_copy(i).wait_send()


def to_lanes(column):
    n = column.shape[0]
    if n < LANES:
        column = jnp.concatenate([column, jnp.zeros((LANES - n, 1), column.dtype)], axis=0)
    return jnp.broadcast_to(column, (LANES, LANES)).T[0, :n]


def place_kernel(
    final, scales, sums, lows, turned,
    gate, up, scale_gate, norm, late_scale,
    late, result, sem, late_sem,
):
    width = scale_gate.shape[0]
    odd = lax.rem(lax.axis_index("zero"), 2)
    early = width // LANES * LANES - LANES
    copies = [
        pltpu.make_async_copy(
            final.at[a, pl.ds(i * height // PIECES, height // PIECES)],
            out.at[pl.ds(i * height // PIECES, height // PIECES)],
            sem.at[a, i],
        )
        for i in range(PIECES)
        for a, (out, height) in enumerate(((gate, width), (up, early)))
    ]
    between = pltpu.make_async_copy(
        final.at[1, pl.ds(early, HALF)], up.at[pl.ds(early, HALF)], late_sem.at[0]
    )
    row = pl.multiple_of(early + HALF * odd, HALF)
    rest = pltpu.make_async_copy(late, up.at[pl.ds(row, LANES)], late_sem.at[1])
    for copy in copies:
        copy.start()
    pl.when(odd == 1)(lambda: between.start())
    for i in range(LANES // HALF):
        start = pl.multiple_of(row + HALF * i, HALF)
        high = turned[1, pl.ds(pl.multiple_of(start + HALF * odd, HALF), HALF), :]
        scale = combine(final.at[1], start, high, lows.at[1], result, late, HALF * i)
        late_scale[pl.ds(HALF * i, HALF), :] = scale
    for k in range(0, width, LANES):
        w = min(LANES, width - k)
        scale_gate[pl.ds(k, w)] = to_lanes(scales[0, pl.ds(k, w), :])
    length = sums.shape[2]
    for i in range(sums.shape[0]):
        norm[pl.ds(i * length, length)] = sums[i, 0].astype(norm.dtype)
    rest.start()
    for copy in copies:
        copy.wait()
    pl.when(odd == 1)(lambda: between.wait())
    rest.wait()


def last_kernel(
    n, up_in, own, from_1, from_2, from_3, lows, turned, scales, late_scale,
    up, scale_up, final, result, sem,
):
    del up_in
    rows, width = own.shape[1], scale_up.shape[0]
    z = lax.axis_index("zero")
    row = pair_row(z, width)
    for j, piece in enumerate((own, from_1, from_2, from_3)):
        start = pl.multiple_of(peer(z, n, n - j) * rows, LANES)
        final[:, pl.ds(start, rows)] = piece[...]
    high = turned[1, pl.ds(pl.multiple_of(row + first_row(z), HALF), HALF), :]
    scale = combine(final, 0, high, lows.at[1], result, final, 0)
    copy = pltpu.make_async_copy(final, up.at[pl.ds(row, HALF)], sem)
    copy.start()
    for k in range(0, width, LANES):
        w = min(LANES, width - k)
        scale_up[pl.ds(k, w)] = to_lanes(scales[1, pl.ds(k, w), :])
    late = to_lanes(late_scale[...])
    for odd, place in ((0, width - HALF), (1, 0)):
        @pl.when(lax.rem(z, 2) == odd)
        def _(odd=odd, place=place):
            scale_up[pl.ds(width - LANES - HALF * (1 - odd), LANES)] = late
            scale_up[pl.ds(place, HALF)] = to_lanes(scale)
    copy.wait()


def exchange(weight_gate, low_gate, high_gate, weight_up, low_up, high_up, norm_train, norm_step):
    n, groups = lax.axis_size("zero"), lax.axis_size("cols")
    rows, width = weight_gate.shape[0], weight_gate.shape[1] // n
    rank, length = low_gate.shape[1], norm_train.shape[0]
    steps = 2 * (width // LANES)
    dma = pltpu.SemaphoreType.DMA
    bf16, f32 = jnp.bfloat16, jnp.float32
    vmem, hbm = pl.BlockSpec(memory_space=pltpu.VMEM), pl.BlockSpec(memory_space=pl.ANY)
    work = pl.CostEstimate(
        flops=4 * width * n * rows * rank,
        bytes_accessed=8 * width * n * rows,
        transcendentals=0,
    )
    final, scales, sums, lows, turned, own, *pieces = pl.pallas_call(
        functools.partial(exchange_kernel, n, groups),
        in_specs=[hbm] * 8,
        out_specs=[vmem] * 5 + [hbm] * n,
        out_shape=[
            pltpu.VMEM((2, width, n * rows), bf16),
            pltpu.VMEM((2, width, 1), f32),
            pltpu.VMEM((n * groups, 1, length), f32),
            pltpu.VMEM((2, n, rank, rows), bf16),
            pltpu.VMEM((2, width + HALF, rank), bf16),
        ]
        + [jax.ShapeDtypeStruct((HALF, rows), bf16)] * n,
        scratch_shapes=[
            pltpu.VMEM((2, n, rows, LANES), bf16),
            pltpu.VMEM((2, n // 2, rows, LANES), bf16),
            pltpu.VMEM((SLOTS, n - 1, LANES, rows), bf16),
            pltpu.VMEM((2, n // 2, LANES, rows), bf16),
            pltpu.VMEM((2, rank, width + HALF), bf16),
            pltpu.VMEM((HALF, n * rows), f32),
            pltpu.VMEM((length,), f32),
            pltpu.VMEM((length,), f32),
            dma((2, n)),
            dma((2, n // 2)),
            dma,
            dma((2,)),
            dma((2,)),
            dma((SLOTS, n - 1)),
            dma((steps, n - 1)),
            dma((n - 1,)),
            dma((n - 1,)),
            dma((4,)),
            dma((n,)),
            dma((2,)),
            dma((n * groups - 1,)),
            dma((n * groups - 1,)),
            dma((n,)),
        ],
        cost_estimate=work,
        compiler_params=pltpu.CompilerParams(
            collective_id=0, has_side_effects=True, vmem_limit_bytes=GRANT
        ),
    )(weight_gate, weight_up, low_gate.T, low_up.T, high_gate, high_up, norm_train, norm_step)
    arrived = [
        lax.ppermute(pieces[j - 1], "zero", [(i, (i + j) % n) for i in range(n)])
        for j in reversed(range(1, n))
    ][::-1]
    final, scales, sums, lows, turned = (
        pltpu.with_memory_space_constraint(v, pltpu.VMEM)
        for v in (final, scales, sums, lows, turned)
    )
    gate, up, scale_gate, norm, late_scale = pl.pallas_call(
        place_kernel,
        in_specs=[vmem] * 5,
        out_specs=[hbm] * 2 + [vmem] * 3,
        out_shape=[
            jax.ShapeDtypeStruct((width, n * rows), bf16),
            jax.ShapeDtypeStruct((width, n * rows), bf16),
            jax.ShapeDtypeStruct((width,), f32),
            jax.ShapeDtypeStruct((n * groups * length,), bf16),
            pltpu.VMEM((LANES, 1), f32),
        ],
        scratch_shapes=[
            pltpu.VMEM((LANES, n * rows), bf16),
            pltpu.VMEM((HALF, n * rows), f32),
            dma((2, PIECES)),
            dma((2,)),
        ],
        cost_estimate=work,
        compiler_params=pltpu.CompilerParams(vmem_limit_bytes=GRANT),
    )(final, scales, sums, lows, turned)
    up, scale_up = pl.pallas_call(
        functools.partial(last_kernel, n),
        in_specs=[hbm] + [vmem] * 8,
        out_specs=[hbm, vmem],
        out_shape=[
            jax.ShapeDtypeStruct((width, n * rows), bf16),
            jax.ShapeDtypeStruct((width,), f32),
        ],
        scratch_shapes=[
            pltpu.VMEM((HALF, n * rows), bf16),
            pltpu.VMEM((HALF, n * rows), f32),
            dma,
        ],
        input_output_aliases={0: 0},
        compiler_params=pltpu.CompilerParams(vmem_limit_bytes=GRANT),
    )(up, own, *arrived, lows, turned, scales, late_scale)
    return gate.T, up.T, scale_gate, scale_up, norm


def local(*args):
    n, groups = lax.axis_size("zero"), lax.axis_size("cols")
    rows, total = args[0].shape
    if n == 4 and groups == 2 and rows % LANES == 0 and (total // n) % LANES == HALF:
        return exchange(*args)
    return general(*args)


def solution(mesh):
    in_specs = (
        P(("unit", "zero"), "cols"),
        P(("unit", "zero"), None),
        P("unit", "cols"),
        P(("unit", "zero"), "cols"),
        P(("unit", "zero"), None),
        P("unit", "cols"),
        P(("unit", "zero", "cols")),
        P(("unit", "zero", "cols")),
    )
    out_specs = (
        P("unit", ("cols", "zero")),
        P("unit", ("cols", "zero")),
        P(("unit", "cols", "zero")),
        P(("unit", "cols", "zero")),
        P("unit"),
    )
    return jax.shard_map(local, mesh=mesh, in_specs=in_specs, out_specs=out_specs, check_vma=False)
```

```python
import functools

import jax
import jax.numpy as jnp
from jax import lax
from jax.experimental import pallas as pl
from jax.experimental.pallas import tpu as pltpu
from jax.sharding import PartitionSpec as P

mix_rate = 0.5


def cuts(units, shares):
    total, marks, seen = sum(shares), [0], 0
    for share in shares:
        seen += share
        marks.append(units * seen // total)
    return [(a, b) for a, b in zip(marks[:-1], marks[1:]) if b > a]


def merge_kernel(block_ref, low_ref, high_ref, *refs):
    final_ref, scale_ref, result_ref = refs[-3:]
    n, _, rows = block_ref.shape
    change = mix_rate * jnp.dot(high_ref[...], low_ref[...], preferred_element_type=jnp.float32)
    total = None
    for s in range(n):
        part = block_ref[s].astype(jnp.float32) + change[:, s * rows : (s + 1) * rows]
        result_ref[:, s * rows : (s + 1) * rows] = part
        size = jnp.sum(jnp.abs(part), axis=1, keepdims=True)
        total = size if total is None else total + size
    scale = total / (n * rows)
    scale_ref[...] = scale
    final_ref[...] = (result_ref[...] / scale).astype(final_ref.dtype)


def merge(block, low, high, final, first, step, width):
    n, part, rows = block.shape
    rank = low.shape[0]
    offset = first // step
    operands = [block, low, high]
    in_specs = [
        pl.BlockSpec((n, step, rows), lambda i: (0, i, 0)),
        pl.BlockSpec((rank, n * rows), lambda i: (0, 0)),
        pl.BlockSpec((step, rank), lambda i: (i + offset, 0)),
    ]
    aliases = {}
    if final is not None:
        operands.append(final)
        in_specs.append(pl.BlockSpec(memory_space=pl.ANY))
        aliases = {3: 0}
    return pl.pallas_call(
        merge_kernel,
        grid=(part // step,),
        in_specs=in_specs,
        out_specs=[
            pl.BlockSpec((step, n * rows), lambda i: (i + offset, 0)),
            pl.BlockSpec((step, 1), lambda i: (i, 0)),
        ],
        out_shape=[
            jax.ShapeDtypeStruct((width, n * rows), jnp.bfloat16),
            jax.ShapeDtypeStruct((part, 1), jnp.float32),
        ],
        scratch_shapes=[pltpu.VMEM((step, n * rows), jnp.float32)],
        input_output_aliases=aliases,
        cost_estimate=pl.CostEstimate(
            flops=2 * part * n * rows * rank,
            bytes_accessed=4 * part * n * rows,
            transcendentals=0,
        ),
        compiler_params=pltpu.CompilerParams(vmem_limit_bytes=24 << 20),
    )(*operands)


def general(weight_gate, low_gate, high_gate, weight_up, low_up, high_up, norm_train, norm_step):
    n = lax.axis_size("zero")
    rows, width = weight_gate.shape[0], weight_gate.shape[1] // n
    rank = low_gate.shape[1]
    place = lax.axis_index("zero")
    step = next(s for s in (48, 24, 16, 8, width) if width % s == 0)

    lows = lax.all_gather(
        jnp.concatenate([low_gate.T, low_up.T], axis=0), "zero", axis=1, tiled=True
    )
    serve_norm = lax.all_gather(
        (norm_train + norm_step).astype(jnp.bfloat16), ("zero", "cols"), axis=0, tiled=True
    )
    lows, serve_norm, weight_gate, weight_up = lax.optimization_barrier(
        (lows, serve_norm, weight_gate, weight_up)
    )
    low = {"gate": lows[:rank], "up": lows[rank:]}
    high = {
        "gate": lax.dynamic_slice_in_dim(high_gate, place * width, width, axis=1).T,
        "up": lax.dynamic_slice_in_dim(high_up, place * width, width, axis=1).T,
    }
    turned = {
        "gate": weight_gate.T.reshape(n, width, rows),
        "up": weight_up.T.reshape(n, width, rows),
    }

    shares = {"gate": (1, 3), "up": (7, 2)}
    jobs = [
        (name, a * step, b * step)
        for name in ("gate", "up")
        for a, b in cuts(width // step, shares[name])
    ]
    finals = {"gate": None, "up": None}
    scales = {"gate": [], "up": []}
    block = None
    arrived = []
    for name, a, b in jobs:
        sent = turned[name][:, a:b]
        if block is not None:
            sent, block = lax.optimization_barrier((sent, block))
            arrived.append(block)
        block = lax.all_to_all(sent, "zero", split_axis=0, concat_axis=0, tiled=True)
    arrived.append(block)
    for (name, a, b), block in zip(jobs, arrived):
        finals[name], scale = merge(block, low[name], high[name], finals[name], a, step, width)
        scales[name].append(scale[:, 0])
    return (
        finals["gate"].T,
        finals["up"].T,
        jnp.concatenate(scales["gate"]),
        jnp.concatenate(scales["up"]),
        serve_norm,
    )


MESH = pl.DeviceIdType.MESH
LANES, HALF, AHEAD, PIECES, GRANT = 128, 64, 4, 4, 22 << 20
SLOTS = AHEAD + 2


def peer(z, n, shift):
    return lax.rem(z + shift, n)


def first_row(d):
    return HALF * lax.rem(d, 2)


def pair_row(d, width):
    return pl.multiple_of((width - HALF) * (1 - lax.rem(d, 2)), HALF)


def enter(places):
    barrier = pltpu.get_barrier_semaphore()
    for place in places:
        pl.semaphore_signal(barrier, inc=1, device_id=place, device_id_type=MESH)
    return lambda: pl.semaphore_wait(barrier, len(places))


def combine(source, row, high, lows, result, target, place):
    n, _, rows = lows.shape
    span = pl.ds(row, HALF)
    size = None
    for s in range(n):
        cut = slice(s * rows, (s + 1) * rows)
        change = mix_rate * jnp.dot(high, lows[s], preferred_element_type=jnp.float32)
        part = source[span, cut].astype(jnp.float32) + change
        result[:, cut] = part
        mine = jnp.sum(jnp.abs(part), axis=1, keepdims=True)
        size = mine if size is None else size + mine
    scale = size / (n * rows)
    inverse = 1.0 / scale
    for s in range(n):
        cut = slice(s * rows, (s + 1) * rows)
        target[pl.ds(place, HALF), cut] = (result[:, cut] * inverse).astype(target.dtype)
    return scale


def exchange_kernel(
    n, groups,
    weight_gate, weight_up, low_gate, low_up, high_gate, high_up, norm_train, norm_step,
    final, scales, sums, lows, turned, near, own_piece, piece_2, piece_3,
    raw, raw_pair, sent, sent_pair, highs, result, train, step,
    raw_sem, pair_sem, low_sem, high_sem, norm_sem,
    send_sem, recv_sem, pair_send, pair_recv, low_send, low_recv, swap_sem, norm_send, norm_recv,
    piece_sem, near_sem,
):
    rows, total = weight_gate.shape
    width = total // n
    mains = width // LANES
    steps = 2 * mains
    weights, own_lows, own_highs = (weight_gate, weight_up), (low_gate, low_up), (high_gate, high_up)
    z, x = lax.axis_index("zero"), lax.axis_index("cols")
    odd = lax.rem(z, 2)
    here = z * groups + x
    lanes = pl.ds(pl.multiple_of(z * rows, LANES), rows)

    def place(i):
        there = lax.rem(here + i, n * groups)
        return {"zero": there // groups, "cols": lax.rem(there, groups)}

    def load(a, s, slot, j):
        d = peer(z, n, j)
        tile = (d // 2) * (2 * width // LANES) + lax.rem(d, 2) * (mains + 1) + s
        start = pl.multiple_of(tile * LANES, LANES)
        return pltpu.make_async_copy(
            weights[a].at[:, pl.ds(start, LANES)], raw.at[slot, j], raw_sem.at[slot, j]
        )

    def start_loads(t):
        def go(a):
            for j in reversed(range(n)):
                load(a, t - a * mains, lax.rem(t, 2), j).start()

        if isinstance(t, int):
            go(t // mains)
        else:
            for a in range(2):
                pl.when(t // mains == a)(functools.partial(go, a))

    def load_pair(a, q):
        tile = q * (2 * width // LANES) + mains
        return pltpu.make_async_copy(
            weights[a].at[:, pl.ds(tile * LANES, LANES)], raw_pair.at[a, q], pair_sem.at[a, q]
        )

    def own_low(a):
        return pltpu.make_async_copy(own_lows[a], lows.at[a, z], low_sem)

    def own_high(a):
        start = pl.multiple_of(z * width - HALF * odd, LANES)
        return pltpu.make_async_copy(
            own_highs[a].at[:, pl.ds(start, width + HALF)], highs.at[a], high_sem.at[a]
        )

    def bulk(t, j):
        d = peer(z, n, j)
        a = t // mains
        row = pl.multiple_of(first_row(d) + LANES * (t - a * mains), HALF)
        slot = lax.rem(t, SLOTS)
        return pltpu.make_async_remote_copy(
            src_ref=sent.at[slot, j - 1],
            dst_ref=final.at[a, pl.ds(row, LANES), lanes],
            send_sem=send_sem.at[slot, j - 1],
            recv_sem=recv_sem.at[t, j - 1],
            device_id={"zero": d},
            device_id_type=MESH,
        )

    def pair_of(a, d):
        return sent_pair.at[a, d // 2, pl.ds(pl.multiple_of(first_row(d), HALF), HALF)]

    def pair(j):
        d = peer(z, n, j)
        return pltpu.make_async_remote_copy(
            src_ref=pair_of(0, d),
            dst_ref=final.at[0, pl.ds(pair_row(d, width), HALF), lanes],
            send_sem=pair_send.at[j - 1],
            recv_sem=pair_recv.at[j - 1],
            device_id={"zero": d},
            device_id_type=MESH,
        )

    def piece_copy(i):
        d, out = ((z, own_piece), (peer(z, n, n // 2), piece_2), (n - 1 - z, piece_3))[i]
        return pltpu.make_async_copy(pair_of(1, d), out, piece_sem.at[i])

    def near_copy():
        return pltpu.make_async_remote_copy(
            src_ref=pair_of(1, mate),
            dst_ref=near,
            send_sem=near_sem.at[0],
            recv_sem=near_sem.at[1],
            device_id={"zero": mate},
            device_id_type=MESH,
        )

    def low_copy(block, d, index):
        return pltpu.make_async_remote_copy(
            src_ref=lows.at[x, block],
            dst_ref=lows.at[x, block],
            send_sem=low_send.at[index],
            recv_sem=low_recv.at[block],
            device_id={"zero": d},
            device_id_type=MESH,
        )

    def low_swap():
        return pltpu.make_async_remote_copy(
            src_ref=lows.at[x],
            dst_ref=lows.at[x],
            send_sem=swap_sem.at[0],
            recv_sem=swap_sem.at[1],
            device_id={"cols": 1 - x},
            device_id_type=MESH,
        )

    def norm_copy(i):
        return pltpu.make_async_remote_copy(
            src_ref=sums.at[here],
            dst_ref=sums.at[here],
            send_sem=norm_send.at[i - 1],
            recv_sem=norm_recv.at[i - 1],
            device_id=place(i),
            device_id_type=MESH,
        )

    def prepare(t, reused):
        slot, from_slot, a = lax.rem(t, SLOTS), lax.rem(t, 2), t // mains
        if reused:
            for j in range(1, n):
                bulk(t - SLOTS, j).wait_send()
        for j in reversed(range(n)):
            load(0, 0, from_slot, j).wait()
            part = raw[from_slot, j].T
            if j:
                sent[slot, j - 1] = part
            else:
                row = pl.multiple_of(first_row(z) + LANES * (t - a * mains), HALF)
                final[a, pl.ds(row, LANES), lanes] = part

    def prepare_pair(a):
        for q in range(n // 2):
            load_pair(a, q).wait()
            sent_pair[a, q] = raw_pair[a, q].T

    def keep_pair(a):
        own = sent_pair[a, z // 2, pl.ds(pl.multiple_of(first_row(z), HALF), HALF), :]
        final[a, pl.ds(pair_row(z, width), HALF), lanes] = own

    def merge_at(a, row):
        row = pl.multiple_of(row, HALF)
        high = turned[a, pl.ds(pl.multiple_of(row + HALF * odd, HALF), HALF), :]
        scale = combine(final.at[a], row, high, lows.at[a], result, final.at[a], row)
        scales[a, pl.ds(row, HALF), :] = scale

    def finish(t):
        for j in range(1, n):
            bulk(t, j).wait_recv()
        a = t // mains
        row = first_row(z) + LANES * (t - a * mains)
        lax.fori_loop(0, LANES // HALF, lambda i, c: (merge_at(a, row + HALF * i), c)[1], 0)

    def send(t):
        for j in reversed(range(1, n)):
            bulk(t, j).start()

    wait_for_all = enter([place(i) for i in range(1, n * groups)])
    for a in range(2):
        pl.when(x == a)(lambda a=a: own_low(a).start())
    for q in range(n // 2):
        load_pair(0, q).start()
    start_loads(0)
    start_loads(1)
    norm_loads = [
        pltpu.make_async_copy(norm_train, train, norm_sem.at[0]),
        pltpu.make_async_copy(norm_step, step, norm_sem.at[1]),
    ]
    for copy in norm_loads:
        copy.start()
    for a in range(2):
        own_high(a).start()
    for q in range(n // 2):
        load_pair(1, q).start()

    mate, inner = z + 1 - 2 * odd, (z == 1) | (z == 2)
    gateway, other = 2 - z // 2, 2 - 2 * (z // 2)
    own_low(0).wait()
    prepare_pair(0)
    wait_for_all()
    low_copy(z, gateway, 0).start()
    low_copy(z, mate, 1).start()
    for copy in norm_loads:
        copy.wait()
    sums[here] = (train[...] + step[...]).reshape(1, -1)
    for j in reversed(range(1, n)):
        pair(j).start()
    keep_pair(0)
    prepare(0, False)
    start_loads(2)
    for i in range(1, n * groups):
        norm_copy(i).start()
    prepare(1, False)
    start_loads(3)
    send(0)

    @pl.when(inner)
    def _():
        for i in range(2):
            low_copy(other + i, mate, 2 + i).wait_recv()
            low_copy(other + i, mate, 2 + i).start()

    t = 2
    while t < AHEAD + 1:
        prepare(t, False)
        start_loads(t + 2)
        send(t - 1)
        t += 1
    for a in range(2):
        own_high(a).wait()
        turned[a] = highs[a].T
    prepare_pair(1)

    low_copy(mate, mate, 0).wait_recv()

    @pl.when(jnp.logical_not(inner))
    def _():
        for i in range(2):
            low_copy(other + i, mate, 2 + i).wait_recv()

    low_swap().start()
    low_swap().wait_recv()
    near_copy().start()
    for i in range(3):
        piece_copy(i).start()
    for j in range(1, n):
        pair(j).wait_recv()
    merge_at(0, pair_row(z, width))

    send(AHEAD)
    prepare(AHEAD + 1, False)
    start_loads(AHEAD + 3)
    finish(0)

    def at(k, carry):
        send(k + AHEAD)
        prepare(k + AHEAD + 1, True)

        @pl.when(k + AHEAD + 3 < steps)
        def _():
            start_loads(k + AHEAD + 3)

        finish(k)
        return carry

    lax.fori_loop(1, steps - AHEAD - 1, at, 0)
    send(steps - 1)
    for i in range(3):
        piece_copy(i).wait()
    near_copy().wait()
    for i in range(1, n * groups):
        norm_copy(i).wait_recv()
    lax.fori_loop(steps - AHEAD - 1, steps - 1, lambda k, c: (finish(k), c)[1], 0)
    for j in range(1, n):
        bulk(steps - 1, j).wait_recv()

    for t in range(steps - SLOTS, steps):
        for j in range(1, n):
            bulk(t, j).wait_send()
    for j in range(1, n):
        pair(j).wait_send()
    low_copy(z, gateway, 0).wait_send()
    low_copy(z, mate, 1).wait_send()

    @pl.when(inner)
    def _():
        for i in range(2):
            low_copy(other + i, mate, 2 + i).wait_send()

    low_swap().wait_send()
    for i in range(1, n * groups):
        norm_copy(i).wait_send()


def to_lanes(column):
    n = column.shape[0]
    if n < LANES:
        column = jnp.concatenate([column, jnp.zeros((LANES - n, 1), column.dtype)], axis=0)
    return jnp.broadcast_to(column, (LANES, LANES)).T[0, :n]


def place_kernel(
    final, scales, sums, lows, turned,
    gate, up, scale_gate, norm, late_scale,
    late, result, sem, late_sem,
):
    width = scale_gate.shape[0]
    odd = lax.rem(lax.axis_index("zero"), 2)
    early = width // LANES * LANES - LANES
    copies = [
        pltpu.make_async_copy(
            final.at[a, pl.ds(i * height // PIECES, height // PIECES)],
            out.at[pl.ds(i * height // PIECES, height // PIECES)],
            sem.at[a, i],
        )
        for i in range(PIECES)
        for a, (out, height) in enumerate(((gate, width), (up, early)))
    ]
    between = pltpu.make_async_copy(
        final.at[1, pl.ds(early, HALF)], up.at[pl.ds(early, HALF)], late_sem.at[0]
    )
    row = pl.multiple_of(early + HALF * odd, HALF)
    rest = pltpu.make_async_copy(late, up.at[pl.ds(row, LANES)], late_sem.at[1])
    for copy in copies:
        copy.start()
    pl.when(odd == 1)(lambda: between.start())
    for i in range(LANES // HALF):
        start = pl.multiple_of(row + HALF * i, HALF)
        high = turned[1, pl.ds(pl.multiple_of(start + HALF * odd, HALF), HALF), :]
        scale = combine(final.at[1], start, high, lows.at[1], result, late, HALF * i)
        late_scale[pl.ds(HALF * i, HALF), :] = scale
    for k in range(0, width, LANES):
        w = min(LANES, width - k)
        scale_gate[pl.ds(k, w)] = to_lanes(scales[0, pl.ds(k, w), :])
    length = sums.shape[2]
    for i in range(sums.shape[0]):
        norm[pl.ds(i * length, length)] = sums[i, 0].astype(norm.dtype)
    rest.start()
    for copy in copies:
        copy.wait()
    pl.when(odd == 1)(lambda: between.wait())
    rest.wait()


def last_kernel(
    n, up_in, near, own, from_2, from_3, lows, turned, scales, late_scale,
    up, scale_up, final, result, sem,
):
    del up_in
    rows, width = own.shape[1], scale_up.shape[0]
    z = lax.axis_index("zero")
    row = pair_row(z, width)
    mate = z + 1 - 2 * lax.rem(z, 2)
    sources = ((z, own), (mate, near), (peer(z, n, n // 2), from_2), (n - 1 - z, from_3))
    for source, piece in sources:
        start = pl.multiple_of(source * rows, LANES)
        final[:, pl.ds(start, rows)] = piece[...]
    high = turned[1, pl.ds(pl.multiple_of(row + first_row(z), HALF), HALF), :]
    scale = combine(final, 0, high, lows.at[1], result, final, 0)
    copy = pltpu.make_async_copy(final, up.at[pl.ds(row, HALF)], sem)
    copy.start()
    for k in range(0, width, LANES):
        w = min(LANES, width - k)
        scale_up[pl.ds(k, w)] = to_lanes(scales[1, pl.ds(k, w), :])
    late = to_lanes(late_scale[...])
    for odd, place in ((0, width - HALF), (1, 0)):
        @pl.when(lax.rem(z, 2) == odd)
        def _(odd=odd, place=place):
            scale_up[pl.ds(width - LANES - HALF * (1 - odd), LANES)] = late
            scale_up[pl.ds(place, HALF)] = to_lanes(scale)
    copy.wait()


def exchange(weight_gate, low_gate, high_gate, weight_up, low_up, high_up, norm_train, norm_step):
    n, groups = lax.axis_size("zero"), lax.axis_size("cols")
    rows, width = weight_gate.shape[0], weight_gate.shape[1] // n
    rank, length = low_gate.shape[1], norm_train.shape[0]
    steps = 2 * (width // LANES)
    dma = pltpu.SemaphoreType.DMA
    bf16, f32 = jnp.bfloat16, jnp.float32
    vmem, hbm = pl.BlockSpec(memory_space=pltpu.VMEM), pl.BlockSpec(memory_space=pl.ANY)
    work = pl.CostEstimate(
        flops=4 * width * n * rows * rank,
        bytes_accessed=8 * width * n * rows,
        transcendentals=0,
    )
    final, scales, sums, lows, turned, near, own, *pieces = pl.pallas_call(
        functools.partial(exchange_kernel, n, groups),
        in_specs=[hbm] * 8,
        out_specs=[vmem] * 6 + [hbm] * 3,
        out_shape=[
            pltpu.VMEM((2, width, n * rows), bf16),
            pltpu.VMEM((2, width, 1), f32),
            pltpu.VMEM((n * groups, 1, length), f32),
            pltpu.VMEM((2, n, rank, rows), bf16),
            pltpu.VMEM((2, width + HALF, rank), bf16),
            pltpu.VMEM((HALF, rows), bf16),
        ]
        + [jax.ShapeDtypeStruct((HALF, rows), bf16)] * 3,
        scratch_shapes=[
            pltpu.VMEM((2, n, rows, LANES), bf16),
            pltpu.VMEM((2, n // 2, rows, LANES), bf16),
            pltpu.VMEM((SLOTS, n - 1, LANES, rows), bf16),
            pltpu.VMEM((2, n // 2, LANES, rows), bf16),
            pltpu.VMEM((2, rank, width + HALF), bf16),
            pltpu.VMEM((HALF, n * rows), f32),
            pltpu.VMEM((length,), f32),
            pltpu.VMEM((length,), f32),
            dma((2, n)),
            dma((2, n // 2)),
            dma,
            dma((2,)),
            dma((2,)),
            dma((SLOTS, n - 1)),
            dma((steps, n - 1)),
            dma((n - 1,)),
            dma((n - 1,)),
            dma((4,)),
            dma((n,)),
            dma((2,)),
            dma((n * groups - 1,)),
            dma((n * groups - 1,)),
            dma((3,)),
            dma((2,)),
        ],
        cost_estimate=work,
        compiler_params=pltpu.CompilerParams(
            collective_id=0, has_side_effects=True, vmem_limit_bytes=GRANT
        ),
    )(weight_gate, weight_up, low_gate.T, low_up.T, high_gate, high_up, norm_train, norm_step)
    arrived = [
        lax.ppermute(pieces[0], "zero", [(i, (i + n // 2) % n) for i in range(n)]),
        lax.ppermute(pieces[1], "zero", [(i, n - 1 - i) for i in range(n)]),
    ]
    final, scales, sums, lows, turned, near = (
        pltpu.with_memory_space_constraint(v, pltpu.VMEM)
        for v in (final, scales, sums, lows, turned, near)
    )
    gate, up, scale_gate, norm, late_scale = pl.pallas_call(
        place_kernel,
        in_specs=[vmem] * 5,
        out_specs=[hbm] * 2 + [vmem] * 3,
        out_shape=[
            jax.ShapeDtypeStruct((width, n * rows), bf16),
            jax.ShapeDtypeStruct((width, n * rows), bf16),
            jax.ShapeDtypeStruct((width,), f32),
            jax.ShapeDtypeStruct((n * groups * length,), bf16),
            pltpu.VMEM((LANES, 1), f32),
        ],
        scratch_shapes=[
            pltpu.VMEM((LANES, n * rows), bf16),
            pltpu.VMEM((HALF, n * rows), f32),
            dma((2, PIECES)),
            dma((2,)),
        ],
        cost_estimate=work,
        compiler_params=pltpu.CompilerParams(vmem_limit_bytes=GRANT),
    )(final, scales, sums, lows, turned)
    up, scale_up = pl.pallas_call(
        functools.partial(last_kernel, n),
        in_specs=[hbm] + [vmem] * 8,
        out_specs=[hbm, vmem],
        out_shape=[
            jax.ShapeDtypeStruct((width, n * rows), bf16),
            jax.ShapeDtypeStruct((width,), f32),
        ],
        scratch_shapes=[
            pltpu.VMEM((HALF, n * rows), bf16),
            pltpu.VMEM((HALF, n * rows), f32),
            dma,
        ],
        input_output_aliases={0: 0},
        compiler_params=pltpu.CompilerParams(vmem_limit_bytes=GRANT),
    )(up, near, own, *arrived, lows, turned, scales, late_scale)
    return gate.T, up.T, scale_gate, scale_up, norm


def local(*args):
    n, groups = lax.axis_size("zero"), lax.axis_size("cols")
    rows, total = args[0].shape
    if n == 4 and groups == 2 and rows % LANES == 0 and (total // n) % LANES == HALF:
        return exchange(*args)
    return general(*args)


def solution(mesh):
    in_specs = (
        P(("unit", "zero"), "cols"),
        P(("unit", "zero"), None),
        P("unit", "cols"),
        P(("unit", "zero"), "cols"),
        P(("unit", "zero"), None),
        P("unit", "cols"),
        P(("unit", "zero", "cols")),
        P(("unit", "zero", "cols")),
    )
    out_specs = (
        P("unit", ("cols", "zero")),
        P("unit", ("cols", "zero")),
        P(("unit", "cols", "zero")),
        P(("unit", "cols", "zero")),
        P("unit"),
    )
    return jax.shard_map(local, mesh=mesh, in_specs=in_specs, out_specs=out_specs, check_vma=False)
```
